32 devices in a mesh: rows: 8 (over z, y), trees: 4 (over x, core).
Axes of the slice: x: 2, y: 2, z: 4, core: 2. Of those that a mesh axis runs over, the one named last changes fastest.
Arguments:
- node_of_row: int32 [4, 16384], P('trees', 'rows'), may hold values from 0 to 63
- bag_weight: int32 [4, 16384], P('trees', 'rows'), may hold values from 0 to 6, as said below
- smaller_side: int32 [4, 32], P('trees'), may hold values from 0 to 1
- bins: int32 [16384, 256], P('rows'), may hold values from 0 to 31
- target: float32 [16384], P('rows'), may hold values from -6 to 6
- parent_hist: float32 [4, 256, 3072], P('trees', 'rows')
Outputs:
- child_hist: float32 [4, 256, 6144], P('trees', 'rows')
- best_gain: float32 [4, 64], P('trees')
- importance: float32 [256], P('rows')
The draws below stay inside these ranges and needn't reach their ends.
Inputs may be any that keep to these rules, and one draw needn't show every extreme that they name: `bag_weight`: poisson weights with mean one.
All inputs are finite; a program needn't handle non-finite values.
Results may differ from the reference program's by a relative error of at most 0.002.
Values sent between devices are 32-bit elements; how exact they have to be, the bound alone decides.
A program may use at most 64 MiB of HBM per device.

```python
import math
import jax
import jax.numpy as jnp
import numpy as np
from jax import lax

FEAT = 256
BINS = 32
PAIRS = 32
ROWS = 16384
TREES = 4


def draw_bag_weight(key, part):
    drawn = jax.random.randint(jax.random.fold_in(key, 11), (TREES, ROWS), 0, 1 << 20)
    limits = jnp.array([385749, 771499, 964396, 1028631, 1044680, 1047956], jnp.int32)
    return jnp.sum((drawn[..., None] >= limits).astype(jnp.int32), axis=-1).astype(jnp.int32)


def draw_parent_hist(key, part):
    first, second, third = jax.random.split(jax.random.fold_in(key, 23), 3)
    shape = (TREES, FEAT, BINS, PAIRS)
    middle = ROWS / (2.0 * PAIRS * BINS)
    counts = middle * jax.random.uniform(first, shape, jnp.float32, 0.3, 2.5)
    sums = jax.random.normal(second, shape, jnp.float32) * jnp.sqrt(middle + 1.0)
    squares = counts * jax.random.uniform(third, shape, jnp.float32, 0.5, 2.0)
    stacked = jnp.stack([counts, sums, squares], axis=-1)
    return stacked.reshape(TREES, FEAT, BINS * PAIRS * 3).astype(jnp.float32)


def touch_ends(values, rng, low, high):
    spot = [jax.random.randint(jax.random.fold_in(rng, axis), (), 0, length) for axis, length in enumerate(values.shape)]
    widest = values.shape.index(max(values.shape))
    beside = spot[:widest] + [(spot[widest] + 1) % values.shape[widest]] + spot[widest + 1:]
    return values.at[tuple(spot)].set(low).at[tuple(beside)].set(high)


def shard_levels(stream_key, shape, pieces, low, largest):
    loudness, own = 1.0, jax.random.fold_in(stream_key, 6)
    for axis_at, blocks in pieces:
        draws = jnp.exp(jax.random.uniform(jax.random.fold_in(own, axis_at), (blocks,), jnp.float32, low / len(pieces), largest / len(pieces)))
        loudness = loudness * jnp.repeat(draws, shape[axis_at] // blocks).reshape([-1 if axis == axis_at else 1 for axis in range(len(shape))])
    return loudness


def rank_bounds(number_of, lean):
    portions = [(1 << 20) // math.isqrt(rank ** lean) + 1 for rank in range(1, number_of + 1)]
    scale = 1 + sum(portions) // (1 << 30)
    return np.cumsum(np.array([max(1, weight // scale) for weight in portions]))


def skewed_ids(rng, extent, number_of, lean):
    listing = rank_bounds(number_of, lean)
    lot = jax.random.randint(jax.random.fold_in(rng, 1), extent, 0, int(listing[number_of - 1]))
    standing = jnp.searchsorted(jnp.asarray(listing, jnp.int32), lot, side="right")
    return jax.random.permutation(jax.random.fold_in(rng, 2), number_of)[standing].astype(jnp.int32)


def scatter_about(key, shape, spread, most, cuts=(), held_as=jnp.bfloat16):
    level = shard_levels(key, shape, cuts, -0.22, 0.18) if cuts else 1.0
    values = jax.random.normal(key, shape, jnp.float32) * spread * level
    return jnp.minimum(jnp.maximum(values, -most), most).astype(held_as)


def setup_inputs(seed: int = 0) -> dict:
    splits = jax.random.split(jax.random.key(seed), 7)
    return {
        "node_of_row": touch_ends(skewed_ids(splits[0], (TREES, ROWS), 2 * PAIRS, 2), jax.random.fold_in(splits[0], 3), 0, (2 * PAIRS) - 1).astype(jnp.int32),
        "bag_weight": draw_bag_weight(jax.random.fold_in(splits[6], 71), 0),
        "smaller_side": touch_ends(jax.random.randint(splits[2], (TREES, PAIRS), 0, 2), jax.random.fold_in(splits[2], 1), 0, 1).astype(jnp.int32),
        "bins": touch_ends(jax.random.randint(splits[3], (ROWS, FEAT), 0, BINS), jax.random.fold_in(splits[3], 1), 0, BINS - 1).astype(jnp.int32),
        "target": scatter_about(splits[4], (ROWS,), 1.0, 6.0, ((0, 8),), jnp.float32),
        "parent_hist": draw_parent_hist(jax.random.fold_in(splits[6], 71), 0),
    }


def tree_small(nodes, weights, flags, bins, target):
    pair = nodes // 2
    side = nodes % 2
    keep = (side == flags[pair]).astype(jnp.float32)
    wk = weights.astype(jnp.float32) * keep
    stats = jnp.stack([wk, wk * target, wk * target * target], axis=1).astype(jnp.bfloat16).astype(jnp.float32)
    width = min(FEAT, 32)

    def block(index):
        cols = lax.dynamic_slice_in_dim(bins, (index * width).astype(jnp.int32), width, 1)
        fidx = jnp.arange(width, dtype=jnp.int32)
        ids = (fidx[None, :] * BINS + cols) * PAIRS + pair[:, None]
        data = jnp.broadcast_to(stats[:, None, :], (stats.shape[0], width, 3))
        summed = jax.ops.segment_sum(data.reshape(-1, 3), ids.reshape(-1), num_segments=width * BINS * PAIRS)
        return summed.reshape(width, BINS, PAIRS, 3)

    blocks = lax.map(block, jnp.arange(FEAT // width, dtype=jnp.int32))
    return blocks.reshape(FEAT, BINS, PAIRS, 3)


def gains_of(children):
    count = children[..., 0]
    total = children[..., 1]
    ccum = jnp.cumsum(count, axis=1)
    scum = jnp.cumsum(total, axis=1)
    call = ccum[:, -1:, :]
    sall = scum[:, -1:, :]
    left_c = ccum[:, :-1, :]
    left_s = scum[:, :-1, :]
    gain = left_s * left_s / (jnp.maximum(left_c, 0.0) + 1.0)
    gain = gain + (sall - left_s) ** 2 / (jnp.maximum(call - left_c, 0.0) + 1.0)
    gain = gain - sall * sall / (jnp.maximum(call, 0.0) + 1.0)
    return jnp.max(gain, axis=1)


def reference(node_of_row, bag_weight, smaller_side, bins, target, parent_hist):
    hists = []
    bests = []
    featsum = jnp.zeros((FEAT,), jnp.float32)
    for tree in range(TREES):
        small = tree_small(node_of_row[tree], bag_weight[tree], smaller_side[tree], bins, target)
        parent = parent_hist[tree].reshape(FEAT, BINS, PAIRS, 3)
        sibling = parent - small
        take = (jnp.arange(2, dtype=jnp.int32)[None, :] == smaller_side[tree][:, None])
        children = jnp.where(take[None, None, :, :, None], small[:, :, :, None, :], sibling[:, :, :, None, :])
        children = children.reshape(FEAT, BINS, 2 * PAIRS, 3)
        hists.append(children.reshape(FEAT, BINS * 2 * PAIRS * 3))
        fgain = gains_of(children)
        bests.append(jnp.max(fgain, axis=0))
        featsum = featsum + jnp.sum(fgain, axis=1)
    importance = featsum / (TREES * 2 * PAIRS)
    return jnp.stack(hists), jnp.stack(bests), importance
```

```python
import functools
import math

import jax
import jax.numpy as jnp
from jax import lax
from jax.experimental import pallas as pl
from jax.experimental.pallas import tpu as pltpu
from jax.sharding import PartitionSpec as P

BINS = 32
MESH = pl.DeviceIdType.MESH
HIGH = lax.Precision.HIGHEST
NT = (((1,), (1,)), ((), ()))


def kernel(
    R, T, owned, nbins, pairs, nrows,
    node_ref, wgt_ref, flag_ref, bins_ref, target_ref, parent_ref,
    child_ref, small_ref,
    *scratch,
):
    rows = nbins // 4 * owned
    acc = pltpu.ACC
    spec = lambda q, m: acc(q)((m, 256), jnp.float32)
    pl.run_scoped(
        functools.partial(
            body, R, T, owned, nbins, pairs, nrows,
            node_ref, wgt_ref, flag_ref, bins_ref, target_ref, parent_ref, child_ref, small_ref, *scratch
        ),
        spec(0, rows), spec(0, rows), spec(1, rows), spec(1, rows), spec(0, 16), spec(1, 16),
    )


def body(
    R, T, owned, nbins, pairs, nrows,
    node_ref, wgt_ref, flag_ref, bins_ref, target_ref, parent_ref,
    child_ref, small_ref,
    node_v, wgt_v, flag_v, bins_v, own_v, own_t, sendbuf, recv, stat_v, par_v, acc, spread, tn_v, sg_v,
    msg_b, got_b, msg_i, got_i,
    in_sem, d_send, d_recv, s_send, s_recv, y_send, x_send, x_recv, p_send, p_recv, q_send, q_recv,
    b_send, b_recv, i_send, i_recv,
    acc0, acc1, acc2, acc3, idle0, idle1,
):
    f32, bf16, i32 = jnp.float32, jnp.bfloat16, jnp.int32
    accs = (acc0, acc1, acc2, acc3)
    r = lax.axis_index("rows")
    t = lax.axis_index("trees")
    tp = t + 1 - 2 * lax.rem(t, 2)
    tx = lax.rem(t + T // 2, T)
    tpx = lax.rem(tp + T // 2, T)
    quarter = nrows // T
    width = 6 * pairs
    groups = nbins // 4

    bins_in = pltpu.make_async_copy(
        bins_ref.at[pl.ds(pl.multiple_of(t * quarter, quarter), quarter), :], bins_v, in_sem.at[0]
    )
    bins_in.start()
    node_in = pltpu.make_async_copy(node_ref, node_v, in_sem.at[2])
    wgt_in = pltpu.make_async_copy(wgt_ref, wgt_v, in_sem.at[3])
    target_in = pltpu.make_async_copy(target_ref, stat_v.at[r, :, pl.ds(2 * nrows, nrows)], in_sem.at[4])
    node_in.start()
    wgt_in.start()
    target_in.start()
    flag_in = pltpu.make_async_copy(flag_ref, flag_v, in_sem.at[5])
    flag_in.start()
    own_in = pltpu.make_async_copy(
        bins_ref.at[:, pl.ds(pl.multiple_of(r * owned // 128 * 128, 128), 128)], own_v, in_sem.at[6]
    )
    own_in.start()
    par_in = pltpu.make_async_copy(parent_ref, par_v, in_sem.at[1])
    par_in.start()

    barrier = pltpu.get_barrier_semaphore()
    for off in range(1, R):
        pl.semaphore_signal(barrier, inc=1, device_id=(lax.rem(r + off, R), t), device_id_type=MESH)
    for off in range(1, T):
        pl.semaphore_signal(barrier, inc=1, device_id=(r, lax.rem(t + off, T)), device_id_type=MESH)

    node_in.wait()
    wgt_in.wait()
    target_in.wait()
    stat_v[r, :, 0:nrows] = node_v[...].astype(f32)
    stat_v[r, :, nrows : 2 * nrows] = wgt_v[...].astype(f32)
    bins_in.wait()
    sendbuf[...] = bins_v[...].astype(f32).T.reshape(R, owned, quarter)

    def flip(m):
        peer, bit = r, 1
        while bit < R:
            on = lax.rem(m // bit, 2)
            peer = peer + on * bit * (1 - 2 * lax.rem(r // bit, 2))
            bit *= 2
        return peer

    def direct(m, src):
        return pltpu.make_async_remote_copy(
            sendbuf.at[flip(m)],
            recv.at[src, t],
            d_send.at[m],
            d_recv.at[src],
            device_id=(flip(m), t),
            device_id_type=MESH,
        )

    def stats(src, to, send):
        return pltpu.make_async_remote_copy(
            stat_v.at[src], stat_v.at[src], send.at[src], s_recv.at[src], device_id=(to, t), device_id_type=MESH
        )

    def stats_out(m):
        return pltpu.make_async_remote_copy(
            stat_v.at[r], stat_v.at[r], s_send.at[m], s_recv.at[r], device_id=(flip(m), t), device_id_type=MESH
        )

    def relay(src, slot, to, send, got):
        return pltpu.make_async_remote_copy(
            recv.at[src, slot], recv.at[src, slot], send.at[src], got.at[src], device_id=(r, to), device_id_type=MESH
        )

    pl.semaphore_wait(barrier, R + T - 2)

    def launch(m, _):
        @pl.when((m == 1) | (lax.rem(m, 2) == 0))
        def _():
            stats_out(m).start()

        direct(m, r).start()
        return 0

    lax.fori_loop(1, R, launch, 0)

    for a in accs:
        acc[0] = pltpu.matmul_pop(a)
    child_ref[0, 0:16, 0:256] = pltpu.matmul_pop(idle0)
    child_ref[0, 0:16, 0:256] = pltpu.matmul_pop(idle1)
    flag_in.wait()
    flag = flag_v[...].astype(f32)
    c_row = lax.broadcasted_iota(i32, (width, pairs), 0)
    p_col = lax.broadcasted_iota(i32, (width, pairs), 1)
    side_c = jnp.sum(jnp.where(c_row // 6 == p_col, flag, 0.0), axis=1, keepdims=True)
    c_one = lax.broadcasted_iota(i32, (width, 1), 0)
    kid_c = (lax.rem(c_one, 6) // 3).astype(f32)
    node_c = 2.0 * (c_one // 6).astype(f32) + side_c
    sign_c = jnp.where(kid_c == side_c, 1.0, -1.0)
    tn_v[...] = jnp.broadcast_to(node_c, (width, quarter)).astype(bf16)
    sg_v[...] = jnp.broadcast_to(sign_c, (width, quarter)).astype(bf16)
    spread[width:, :] = jnp.zeros((256 - width, quarter), bf16)

    own_in.wait()
    lead = pl.multiple_of(lax.rem(r * owned, 128), owned)
    for q in range(T):
        own_t[q] = own_v[q * quarter : (q + 1) * quarter, :].astype(f32).T
        recv[r, q] = own_t[q, pl.ds(lead, owned), :]

    deep = 12 * pairs
    e_lane = lax.broadcasted_iota(i32, (width, 256), 1)
    e_col = lax.broadcasted_iota(i32, (width, 256), 0)
    par_in.wait()
    for k in range(4):
        base = k // 2 * 128
        want = k * 3 * pairs - base + 3 * (e_col // 6) + lax.rem(e_col, 3)
        pick = jnp.where((e_lane == want) & (sign_c < 0.0), 1.0, 0.0).astype(bf16)
        pick = jnp.concatenate([pick, jnp.zeros((256 - width, 256), bf16)], axis=0)
        pltpu.matmul_push_rhs(pick, staging_register=0, mxu_index=k // 2, transpose=True)
        rest = jnp.concatenate(
            [par_v[0, :, g * deep + base : g * deep + base + 256] for g in range(groups)], axis=0
        )
        for limb in range(3):
            part = rest.astype(bf16)
            pltpu.matmul_acc_lhs(accs[k], part, load_staged_rhs=0 if limb == 0 else None)
            rest = rest - part.astype(f32)

    third = lax.rem(lax.broadcasted_iota(i32, (48, quarter), 0), 3)
    count = R * T

    def place(e):
        u = e - T
        idx = u + jnp.where(u >= 1, 3, 0) + jnp.where(u >= 4, 1, 0)
        idx = idx + jnp.where(u >= 4 * R - 8, 1, 0) + jnp.where(u >= 4 * R - 5, 3, 0)
        k = lax.rem(idx, 4)
        m = idx // 4 + 1 - (k + 1) // 2
        m = jnp.where(e < T, 0, m)
        slot = jnp.where(k == 0, t, jnp.where(k == 1, tx, jnp.where(k == 2, tp, tpx)))
        slot = jnp.where(e < T, e, slot)
        k = jnp.where(e < T, -1, k)
        return m, k, slot

    def lay(src, slot):
        base = pl.multiple_of(slot * quarter, quarter)
        nodes = stat_v[src, :, pl.ds(base, quarter)]
        w = stat_v[src, :, pl.ds(pl.multiple_of(base + nrows, quarter), quarter)]
        y = stat_v[src, :, pl.ds(pl.multiple_of(base + 2 * nrows, quarter), quarter)]
        wy = w * y
        wyy = wy * y
        stat = jnp.where(third == 0, w, jnp.where(third == 1, wy, wyy)).astype(bf16)
        node = jnp.broadcast_to(nodes, (48, quarter)).astype(bf16)
        for g in range(width // 48):
            at = slice(g * 48, (g + 1) * 48)
            spread[at, :] = jnp.where(node == tn_v[at, :], stat, jnp.zeros_like(stat)) * sg_v[at, :]

    def stage(tile, q):
        pltpu.matmul_push_rhs(
            spread[:, tile * 256 : (tile + 1) * 256], staging_register=tile, mxu_index=q, transpose=True
        )

    lay(r, 0)
    for tile in range(2):
        for q in range(2):
            stage(tile, q)

    def step(e, _):
        m, k, slot = place(e)
        src = flip(m)

        @pl.when(k == 0)
        def _():
            direct(m, src).wait_recv()
            relay(src, t, tx, x_send, x_recv).start()
            relay(src, t, tp, p_send, p_recv).start()

        @pl.when(k == 1)
        def _():
            relay(src, tx, tx, x_send, x_recv).wait_recv()
            relay(src, tx, tp, q_send, q_recv).start()

        @pl.when(k == 2)
        def _():
            relay(src, tp, tp, p_send, p_recv).wait_recv()

        @pl.when(k == 3)
        def _():
            relay(src, tpx, tp, q_send, q_recv).wait_recv()

        m2, k2, slot2 = place(jnp.minimum(e + 1, count - 1))
        src2 = flip(m2)

        @pl.when((k2 == 0) & (e + 1 < count))
        def _():
            stats(src2, src2, y_send).wait_recv()

            @pl.when(lax.rem(m2, 2) == 0)
            def _():
                stats(src2, flip(1), y_send).start()

        lay(src2, slot2)
        cols = recv[src, slot].astype(bf16)
        for tile in range(2):
            c = cols[:, tile * 256 : (tile + 1) * 256]
            for j in range(2):
                for q in range(2):
                    a = 2 * q + j
                    hot = jnp.concatenate(
                        [
                            jnp.where(c == jnp.asarray(4 * g + a, bf16), jnp.ones_like(c), jnp.zeros_like(c))
                            for g in range(groups)
                        ],
                        axis=0,
                    )
                    pltpu.matmul_acc_lhs(accs[a], hot, load_staged_rhs=tile if j == 0 else None)
                    if j == 0:
                        stage(tile, q)
        return 0

    lax.fori_loop(0, count, step, 0)
    nothing = jnp.zeros((16, 256), bf16)
    for tile in range(2):
        pltpu.matmul_acc_lhs(idle0, nothing, load_staged_rhs=tile)
        pltpu.matmul_acc_lhs(idle1, nothing, load_staged_rhs=tile)
    for k in range(4):
        acc[k] = pltpu.matmul_pop(accs[k])
    msg_i[...] = pltpu.matmul_pop(idle0)[0:1, 0:128] + pltpu.matmul_pop(idle1)[0:1, 0:128]

    def at(b, h):
        return acc[b % 4, b // 4 * owned : (b // 4 + 1) * owned, h * 128 : (h + 1) * 128]

    def shift(x):
        return pltpu.roll(x, 127, 1)

    lane = lax.broadcasted_iota(i32, (owned, 128), 1)
    per_feature = jnp.zeros((owned, 1), f32)
    for h in range(2):
        total = at(0, h)
        for b in range(1, nbins):
            total = total + at(b, h)
        s_all = shift(total)
        cum = jnp.zeros((owned, 128), f32)
        top = jnp.full((owned, 128), -jnp.inf, f32)
        for b in range(nbins - 1):
            cum = cum + at(b, h)
            s = shift(cum)
            o = s_all - s
            g = s * s / (jnp.maximum(cum, 0.0) + 1.0)
            g = g + o * o / (jnp.maximum(total - cum, 0.0) + 1.0)
            top = jnp.maximum(top, g)
        top = top - s_all * s_all / (jnp.maximum(total, 0.0) + 1.0)
        at_lane = lane + h * 128
        fits = (lax.rem(at_lane, 3) == 0) & (at_lane < width)
        msg_b[:, h * 128 : (h + 1) * 128] = jnp.max(jnp.where(fits, top, -jnp.inf), axis=0, keepdims=True)
        per_feature = per_feature + jnp.sum(jnp.where(fits, top, 0.0), axis=1, keepdims=True)
    msg_i[...] = jnp.broadcast_to(per_feature, (owned, 128)).T[0:1, :] if owned == 128 else jnp.concatenate(
        [jnp.broadcast_to(per_feature, (owned, 128)).T[0:1, :], jnp.zeros((1, 128 - owned), f32)], axis=1
    )
    got_b[r] = msg_b[...]
    got_i[t] = msg_i[...]

    def tell_b(off):
        peer = lax.rem(r + off, R)
        return pltpu.make_async_remote_copy(
            msg_b, got_b.at[r], b_send.at[off], b_recv.at[r], device_id=(peer, t), device_id_type=MESH
        )

    def tell_i(off):
        peer = lax.rem(t + off, T)
        return pltpu.make_async_remote_copy(
            msg_i, got_i.at[t], i_send.at[off], i_recv.at[t], device_id=(r, peer), device_id_type=MESH
        )

    for off in range(1, R):
        tell_b(off).start()
    for off in range(1, T):
        tell_i(off).start()

    low = lane < 64
    for j in range(nbins // 2):
        base = 2 * j * width
        mid, end = pltpu.roll(at(2 * j + 1, 0), 64, 1), pltpu.roll(at(2 * j + 1, 1), 64, 1)
        child_ref[0, :, base : base + 128] = at(2 * j, 0)
        child_ref[0, :, base + 128 : base + 256] = jnp.where(low, at(2 * j, 1), mid)
        child_ref[0, :, base + 256 : base + 384] = jnp.where(low, mid, end)

    def drain(m, _):
        src = flip(m)
        direct(m, r).wait_send()

        @pl.when((m == 1) | (lax.rem(m, 2) == 0))
        def _():
            stats_out(m).wait_send()

        @pl.when(lax.rem(m, 2) == 0)
        def _():
            stats(src, flip(1), y_send).wait_send()

        relay(src, t, tx, x_send, x_recv).wait_send()
        relay(src, t, tp, p_send, p_recv).wait_send()
        relay(src, tx, tp, q_send, q_recv).wait_send()
        return 0

    lax.fori_loop(1, R, drain, 0)

    for off in range(1, T):
        src = lax.rem(t - off + T, T)
        pltpu.make_async_remote_copy(
            msg_i, got_i.at[src], i_send.at[off], i_recv.at[src], device_id=(r, src), device_id_type=MESH
        ).wait_recv()
    for off in range(1, R):
        src = lax.rem(r - off + R, R)
        pltpu.make_async_remote_copy(
            msg_b, got_b.at[src], b_send.at[off], b_recv.at[src], device_id=(src, t), device_id_type=MESH
        ).wait_recv()
    peak = got_b[0]
    for s in range(1, R):
        peak = jnp.maximum(peak, got_b[s])
    small_ref[:, 0:256] = peak
    tally = got_i[0]
    for s in range(1, T):
        tally = tally + got_i[s]
    small_ref[:, 256:384] = tally / (T * 2 * pairs)
    for off in range(1, T):
        tell_i(off).wait_send()
    for off in range(1, R):
        tell_b(off).wait_send()


def finish(owned, pairs, child_in, small_in, child_ref, best_ref, imp_ref, sem):
    out = pltpu.make_async_copy(child_in, child_ref, sem)
    out.start()
    width = 6 * pairs
    n_i = lax.broadcasted_iota(jnp.int32, (2 * pairs, width), 0)
    c_i = lax.broadcasted_iota(jnp.int32, (2 * pairs, width), 1)
    take = jnp.where(c_i == 3 * n_i, 1.0, 0.0)
    held = lax.rem(lax.broadcasted_iota(jnp.int32, (8, width), 1), 3) == 0
    peak = jnp.where(held, jnp.broadcast_to(small_in[:, 0:width], (8, width)), 0.0)
    best = lax.dot_general(peak, take, NT, precision=HIGH, preferred_element_type=jnp.float32)
    best_ref[...] = best[0:1, :]
    imp_ref[...] = small_in[:, 256 : 256 + owned]
    out.wait()


def fused(R, T, node_of_row, bag_weight, smaller_side, bins, target, parent_hist):
    nrows, feat = bins.shape
    pairs = smaller_side.shape[1]
    owned = feat // R
    quarter = nrows // T
    width = 6 * pairs
    f32, bf16 = jnp.float32, jnp.bfloat16
    vmem = pl.BlockSpec(memory_space=pltpu.VMEM)
    hbm = pl.BlockSpec(memory_space=pl.ANY)
    dma = pltpu.SemaphoreType.DMA
    child, small = pl.pallas_call(
        functools.partial(kernel, R, T, owned, BINS, pairs, nrows),
        out_shape=(pltpu.VMEM((1, owned, BINS * width), f32), pltpu.VMEM((1, 384), f32)),
        in_specs=[hbm, hbm, hbm, hbm, hbm, hbm],
        out_specs=(vmem, vmem),
        scratch_shapes=[
            pltpu.VMEM((1, nrows), jnp.int32),
            pltpu.VMEM((1, nrows), jnp.int32),
            pltpu.VMEM((1, pairs), jnp.int32),
            pltpu.VMEM((quarter, feat), jnp.int32),
            pltpu.VMEM((nrows, 128), jnp.int32),
            pltpu.VMEM((T, 128, quarter), f32),
            pltpu.VMEM((R, owned, quarter), f32),
            pltpu.VMEM((R, T, owned, quarter), f32),
            pltpu.VMEM((R, 1, 3 * nrows), f32),
            pltpu.VMEM((1, owned, BINS * 3 * pairs), f32),
            pltpu.VMEM((4, BINS // 4 * owned, 256), f32),
            pltpu.VMEM((256, quarter), bf16),
            pltpu.VMEM((width, quarter), bf16),
            pltpu.VMEM((width, quarter), bf16),
            pltpu.VMEM((1, 256), f32),
            pltpu.VMEM((R, 1, 256), f32),
            pltpu.VMEM((1, 128), f32),
            pltpu.VMEM((T, 1, 128), f32),
            dma((7,)), dma((R,)),
            dma((R,)), dma((R,)), dma((R,)), dma((R,)),
            dma((R,)), dma((R,)), dma((R,)), dma((R,)), dma((R,)), dma((R,)),
            dma((R,)), dma((R,)), dma((T,)), dma((T,)),
        ],
        compiler_params=pltpu.CompilerParams(collective_id=0, has_side_effects=True),
    )(*[pltpu.with_memory_space_constraint(x, pltpu.HBM) for x in (node_of_row, bag_weight, smaller_side, bins, target.reshape(1, nrows), parent_hist)])
    child, best, imp = pl.pallas_call(
        functools.partial(finish, owned, pairs),
        out_shape=(
            jax.ShapeDtypeStruct((1, owned, BINS * width), f32),
            jax.ShapeDtypeStruct((1, 2 * pairs), f32),
            jax.ShapeDtypeStruct((1, owned), f32),
        ),
        in_specs=[vmem, vmem],
        out_specs=(hbm, vmem, vmem),
        scratch_shapes=[dma],
        compiler_params=pltpu.CompilerParams(vmem_limit_bytes=8 << 20),
    )(pltpu.with_memory_space_constraint(child, pltpu.VMEM), pltpu.with_memory_space_constraint(small, pltpu.VMEM))
    return child, best, imp.reshape(owned)


def plain(node_of_row, bag_weight, smaller_side, bins, target, parent_hist):
    nrows = bins.shape[0]
    feat = bins.shape[1]
    pairs = smaller_side.shape[1]
    nbins = BINS
    nodes = node_of_row[0]
    flags = smaller_side[0]
    pair = nodes // 2
    side = nodes % 2
    pair_hot = pair[:, None] == jnp.arange(pairs, dtype=jnp.int32)[None, :]
    flag_row = jnp.sum(jnp.where(pair_hot, flags[None, :], 0), axis=1)
    keep = (side == flag_row).astype(jnp.float32)
    wk = bag_weight[0].astype(jnp.float32) * keep
    stats = jnp.stack([wk, wk * target, wk * target * target], axis=1).astype(jnp.bfloat16)
    spread = (pair_hot.astype(jnp.bfloat16)[:, :, None] * stats[:, None, :]).reshape(nrows, pairs * 3)
    levels = jnp.arange(nbins, dtype=jnp.int32)
    owned = feat // lax.axis_size("rows")
    width = math.gcd(lax.axis_size("rows") * owned, 32)

    def one_block(index):
        cols = lax.dynamic_slice_in_dim(bins, index * width, width, 1)
        onehot = (
            (cols[:, :, None] == levels[None, None, :]).astype(jnp.bfloat16).reshape(nrows, width * nbins)
        )
        part = jnp.einsum("rk,rm->km", onehot, spread, preferred_element_type=jnp.float32)
        return part.reshape(width, nbins * pairs * 3)

    blocks = lax.map(one_block, jnp.arange(lax.axis_size("rows") * owned // width, dtype=jnp.int32))
    small = lax.psum_scatter(
        blocks.reshape(lax.axis_size("rows") * owned, nbins * pairs * 3), "rows", scatter_dimension=0, tiled=True
    )
    small = small.reshape(owned, nbins, pairs, 3)
    parent = parent_hist[0].reshape(owned, nbins, pairs, 3)
    sibling = parent - small
    take = jnp.arange(2, dtype=jnp.int32)[None, :] == flags[:, None]
    children = jnp.where(take[None, None, :, :, None], small[:, :, :, None, :], sibling[:, :, :, None, :])
    children = children.reshape(owned, nbins, 2 * pairs, 3)
    ccum = jnp.cumsum(children[..., 0], axis=1)
    scum = jnp.cumsum(children[..., 1], axis=1)
    call = ccum[:, -1:, :]
    sall = scum[:, -1:, :]
    left_c = ccum[:, :-1, :]
    left_s = scum[:, :-1, :]
    gain = left_s * left_s / (jnp.maximum(left_c, 0.0) + 1.0)
    gain = gain + (sall - left_s) ** 2 / (jnp.maximum(call - left_c, 0.0) + 1.0)
    gain = gain - sall * sall / (jnp.maximum(call, 0.0) + 1.0)
    fgain = jnp.max(gain, axis=1)
    best = lax.pmax(jnp.max(fgain, axis=0), "rows")
    featsum = lax.psum(jnp.sum(fgain, axis=1), "trees")
    importance = featsum / (lax.axis_size("trees") * node_of_row.shape[0] * 2 * pairs)
    child_hist = children.reshape(owned, nbins * 2 * pairs * 3)
    return (child_hist[None], best[None], importance)


def solution(mesh):
    R, T = mesh.shape["rows"], mesh.shape["trees"]

    def shards(node_of_row, bag_weight, smaller_side, bins, target, parent_hist):
        nrows, feat = bins.shape
        pairs = smaller_side.shape[1]
        owned = feat // R
        fits = T == 4 and R % 2 == 0 and R & (R - 1) == 0 and node_of_row.shape[0] == 1
        fits = fits and R >= 4 and owned in (16, 32) and feat % 128 == 0 and nrows == T * 512
        fits = fits and pairs == 32 and R * nrows * owned * 4 <= 4 << 20
        body = functools.partial(fused, R, T) if fits else plain
        return body(node_of_row, bag_weight, smaller_side, bins, target, parent_hist)

    return jax.shard_map(
        shards,
        mesh=mesh,
        in_specs=(
            P("trees", "rows"),
            P("trees", "rows"),
            P("trees", None),
            P("rows", None),
            P("rows"),
            P("trees", "rows", None),
        ),
        out_specs=(P("trees", "rows", None), P("trees", None), P("rows")),
        check_vma=False,
    )
```

```python
import functools
import math

import jax
import jax.numpy as jnp
from jax import lax
from jax.experimental import pallas as pl
from jax.experimental.pallas import tpu as pltpu
from jax.sharding import PartitionSpec as P

BINS = 32
MESH = pl.DeviceIdType.MESH
HIGH = lax.Precision.HIGHEST
NT = (((1,), (1,)), ((), ()))


def kernel(
    R, T, owned, nbins, pairs, nrows,
    node_ref, wgt_ref, flag_ref, bins_ref, target_ref, parent_ref,
    child_ref, small_ref,
    *scratch,
):
    rows = nbins // 4 * owned
    acc = pltpu.ACC
    spec = lambda q, m: acc(q)((m, 256), jnp.float32)
    pl.run_scoped(
        functools.partial(
            body, R, T, owned, nbins, pairs, nrows,
            node_ref, wgt_ref, flag_ref, bins_ref, target_ref, parent_ref, child_ref, small_ref, *scratch
        ),
        spec(0, rows), spec(0, rows), spec(1, rows), spec(1, rows), spec(0, 16), spec(1, 16),
    )


def body(
    R, T, owned, nbins, pairs, nrows,
    node_ref, wgt_ref, flag_ref, bins_ref, target_ref, parent_ref,
    child_ref, small_ref,
    node_v, wgt_v, target_v, flag_v, bins_v, own_v, own_t, sendbuf, recv, stat_v, par_v, acc, spread, tn_v, sg_v,
    msg_b, got_b, msg_i, got_i,
    in_sem, d_send, d_recv, s_send, s_recv, y_send, x_send, x_recv, p_send, p_recv, q_send, q_recv,
    b_send, b_recv, i_send, i_recv,
    acc0, acc1, acc2, acc3, idle0, idle1,
):
    f32, bf16, i32 = jnp.float32, jnp.bfloat16, jnp.int32
    accs = (acc0, acc1, acc2, acc3)
    r = lax.axis_index("rows")
    t = lax.axis_index("trees")
    tp = t + 1 - 2 * lax.rem(t, 2)
    tx = lax.rem(t + T // 2, T)
    tpx = lax.rem(tp + T // 2, T)
    quarter = nrows // T
    width = 6 * pairs
    groups = nbins // 4

    bins_in = pltpu.make_async_copy(
        bins_ref.at[pl.ds(pl.multiple_of(t * quarter, quarter), quarter), :], bins_v, in_sem.at[0]
    )
    bins_in.start()
    node_in = pltpu.make_async_copy(node_ref, node_v, in_sem.at[2])
    wgt_in = pltpu.make_async_copy(wgt_ref, wgt_v, in_sem.at[3])
    target_in = pltpu.make_async_copy(target_ref, target_v, in_sem.at[4])
    node_in.start()
    wgt_in.start()
    target_in.start()
    flag_in = pltpu.make_async_copy(flag_ref, flag_v, in_sem.at[5])
    flag_in.start()
    own_in = pltpu.make_async_copy(
        bins_ref.at[:, pl.ds(pl.multiple_of(r * owned // 128 * 128, 128), 128)], own_v, in_sem.at[6]
    )
    own_in.start()
    par_in = pltpu.make_async_copy(parent_ref, par_v, in_sem.at[1])
    par_in.start()

    barrier = pltpu.get_barrier_semaphore()
    for off in range(1, R):
        pl.semaphore_signal(barrier, inc=1, device_id=(lax.rem(r + off, R), t), device_id_type=MESH)
    for off in range(1, T):
        pl.semaphore_signal(barrier, inc=1, device_id=(r, lax.rem(t + off, T)), device_id_type=MESH)

    node_in.wait()
    wgt_in.wait()
    target_in.wait()
    lines = nrows // 128
    for n, held in enumerate((node_v, wgt_v, target_v)):
        for i in range(lines):
            stat_v[r, n * lines + i : n * lines + i + 1, :] = held[:, i * 128 : (i + 1) * 128].astype(f32)
    bins_in.wait()
    sendbuf[...] = bins_v[...].astype(f32).T.reshape(R, owned, quarter)

    def flip(m):
        peer, bit = r, 1
        if isinstance(m, int):
            while bit < R:
                if m // bit % 2:
                    peer = peer + bit * (1 - 2 * lax.rem(r // bit, 2))
                bit *= 2
        while bit < R:
            on = lax.rem(m // bit, 2)
            peer = peer + on * bit * (1 - 2 * lax.rem(r // bit, 2))
            bit *= 2
        return peer

    def direct(m, src):
        return pltpu.make_async_remote_copy(
            sendbuf.at[flip(m)],
            recv.at[src, t],
            d_send.at[m],
            d_recv.at[src],
            device_id=(flip(m), t),
            device_id_type=MESH,
        )

    def stats(src, to, send):
        return pltpu.make_async_remote_copy(
            stat_v.at[src], stat_v.at[src], send.at[src], s_recv.at[src], device_id=(to, t), device_id_type=MESH
        )

    def stats_out(m):
        return pltpu.make_async_remote_copy(
            stat_v.at[r], stat_v.at[r], s_send.at[m], s_recv.at[r], device_id=(flip(m), t), device_id_type=MESH
        )

    def relay(src, slot, to, send, got):
        return pltpu.make_async_remote_copy(
            recv.at[src, slot], recv.at[src, slot], send.at[src], got.at[src], device_id=(r, to), device_id_type=MESH
        )

    pl.semaphore_wait(barrier, R + T - 2)

    stats_out(1).start()
    for m in range(2, R, 2):
        stats_out(m).start()

    turns = [1, 2, 3] if R == 4 else [1, 2, 3, R - 2, R - 1, *range(4, R - 2)]
    for m in turns:
        direct(m, r).start()

    for a in accs:
        acc[0] = pltpu.matmul_pop(a)
    child_ref[0, 0:16, 0:256] = pltpu.matmul_pop(idle0)
    child_ref[0, 0:16, 0:256] = pltpu.matmul_pop(idle1)
    flag_in.wait()
    flag = flag_v[...].astype(f32)
    c_row = lax.broadcasted_iota(i32, (width, pairs), 0)
    p_col = lax.broadcasted_iota(i32, (width, pairs), 1)
    side_c = jnp.sum(jnp.where(c_row // 6 == p_col, flag, 0.0), axis=1, keepdims=True)
    c_one = lax.broadcasted_iota(i32, (width, 1), 0)
    kid_c = (lax.rem(c_one, 6) // 3).astype(f32)
    node_c = 2.0 * (c_one // 6).astype(f32) + side_c
    sign_c = jnp.where(kid_c == side_c, 1.0, -1.0)
    tn_v[...] = jnp.broadcast_to(node_c, (width, quarter)).astype(bf16)
    sg_v[...] = jnp.broadcast_to(sign_c, (width, quarter)).astype(bf16)
    spread[width:, :] = jnp.zeros((256 - width, quarter), bf16)

    own_in.wait()
    lead = pl.multiple_of(lax.rem(r * owned, 128), owned)
    for q in range(T):
        own_t[q] = own_v[q * quarter : (q + 1) * quarter, :].astype(f32).T
        recv[r, q] = own_t[q, pl.ds(lead, owned), :]

    deep = 12 * pairs
    e_lane = lax.broadcasted_iota(i32, (width, 256), 1)
    e_col = lax.broadcasted_iota(i32, (width, 256), 0)
    par_in.wait()
    for k in range(4):
        base = k // 2 * 128
        want = k * 3 * pairs - base + 3 * (e_col // 6) + lax.rem(e_col, 3)
        pick = jnp.where((e_lane == want) & (sign_c < 0.0), 1.0, 0.0).astype(bf16)
        pick = jnp.concatenate([pick, jnp.zeros((256 - width, 256), bf16)], axis=0)
        pltpu.matmul_push_rhs(pick, staging_register=0, mxu_index=k // 2, transpose=True)
        rest = jnp.concatenate(
            [par_v[0, :, g * deep + base : g * deep + base + 256] for g in range(groups)], axis=0
        )
        for limb in range(3):
            part = rest.astype(bf16)
            pltpu.matmul_acc_lhs(accs[k], part, load_staged_rhs=0 if limb == 0 else None)
            rest = rest - part.astype(f32)

    third = lax.rem(lax.broadcasted_iota(i32, (48, quarter), 0), 3)
    count = R * T

    lags = (0, 3, 1, 4)
    plan = [(0, -1 - k) for k in range(T)]
    for j in range(R - 1 + max(lags)):
        plan += [(turns[j - lag], k) for k, lag in enumerate(lags) if 0 <= j - lag < R - 1]

    def place(e):
        m, k = plan[e]
        return m, k, (t, tx, tp, tpx)[k] if k >= 0 else -1 - k

    def lay(src, slot):
        def line(n):
            at = n * lines + slot * (quarter // 128)
            return jnp.concatenate([stat_v[src, pl.ds(at + i, 1), :] for i in range(quarter // 128)], axis=1)

        nodes, w, y = line(0), line(1), line(2)
        wy = w * y
        wyy = wy * y
        stat = jnp.where(third == 0, w, jnp.where(third == 1, wy, wyy)).astype(bf16)
        node = jnp.broadcast_to(nodes, (48, quarter)).astype(bf16)
        for g in range(width // 48):
            at = slice(g * 48, (g + 1) * 48)
            spread[at, :] = jnp.where(node == tn_v[at, :], stat, jnp.zeros_like(stat)) * sg_v[at, :]

    def stage(tile, q):
        pltpu.matmul_push_rhs(
            spread[:, tile * 256 : (tile + 1) * 256], staging_register=tile, mxu_index=q, transpose=True
        )

    lay(r, 0)
    for tile in range(2):
        for q in range(2):
            stage(tile, q)

    def step(e, _):
        m, k, slot = place(e)
        src = flip(m)

        @pl.when(k == 0)
        def _():
            direct(m, src).wait_recv()
            relay(src, t, tx, x_send, x_recv).start()
            relay(src, t, tp, p_send, p_recv).start()

        @pl.when(k == 1)
        def _():
            relay(src, tx, tx, x_send, x_recv).wait_recv()
            relay(src, tx, tp, q_send, q_recv).start()

        @pl.when(k == 2)
        def _():
            relay(src, tp, tp, p_send, p_recv).wait_recv()

        @pl.when(k == 3)
        def _():
            relay(src, tpx, tp, q_send, q_recv).wait_recv()

        m2, k2, slot2 = place(min(e + 1, count - 1))
        src2 = flip(m2)

        if k2 == 0 and e + 1 < count and m2 % 2 == 1:
            stats(src2, src2, y_send).wait_recv()
            later = turns[turns.index(m2) + 1 :][:1]
            for m in later:
                stats(flip(m), flip(m), y_send).wait_recv()
                stats(flip(m), flip(1), y_send).start()

        lay(src2, slot2)
        cols = recv[src, slot].astype(bf16)
        for tile in range(2):
            c = cols[:, tile * 256 : (tile + 1) * 256]
            for j in range(2):
                for q in range(2):
                    a = 2 * q + j
                    hot = jnp.concatenate(
                        [
                            jnp.where(c == jnp.asarray(4 * g + a, bf16), jnp.ones_like(c), jnp.zeros_like(c))
                            for g in range(groups)
                        ],
                        axis=0,
                    )
                    pltpu.matmul_acc_lhs(accs[a], hot, load_staged_rhs=tile if j == 0 else None)
                    if j == 0:
                        stage(tile, q)
        return 0

    for e in range(count):
        step(e, 0)
    nothing = jnp.zeros((16, 256), bf16)
    for tile in range(2):
        pltpu.matmul_acc_lhs(idle0, nothing, load_staged_rhs=tile)
        pltpu.matmul_acc_lhs(idle1, nothing, load_staged_rhs=tile)
    for k in range(4):
        acc[k] = pltpu.matmul_pop(accs[k])
    msg_i[...] = pltpu.matmul_pop(idle0)[0:1, 0:128] + pltpu.matmul_pop(idle1)[0:1, 0:128]

    def at(b, h):
        return acc[b % 4, b // 4 * owned : (b // 4 + 1) * owned, h * 128 : (h + 1) * 128]

    def shift(x):
        return pltpu.roll(x, 127, 1)

    lane = lax.broadcasted_iota(i32, (owned, 128), 1)
    per_feature = jnp.zeros((owned, 1), f32)
    for h in range(2):
        total = at(0, h)
        for b in range(1, nbins):
            total = total + at(b, h)
        s_all = shift(total)
        cum = jnp.zeros((owned, 128), f32)
        top = jnp.full((owned, 128), -jnp.inf, f32)
        for b in range(nbins - 1):
            cum = cum + at(b, h)
            s = shift(cum)
            o = s_all - s
            g = s * s / (jnp.maximum(cum, 0.0) + 1.0)
            g = g + o * o / (jnp.maximum(total - cum, 0.0) + 1.0)
            top = jnp.maximum(top, g)
        top = top - s_all * s_all / (jnp.maximum(total, 0.0) + 1.0)
        at_lane = lane + h * 128
        fits = (lax.rem(at_lane, 3) == 0) & (at_lane < width)
        msg_b[:, h * 128 : (h + 1) * 128] = jnp.max(jnp.where(fits, top, -jnp.inf), axis=0, keepdims=True)
        per_feature = per_feature + jnp.sum(jnp.where(fits, top, 0.0), axis=1, keepdims=True)
    msg_i[...] = jnp.broadcast_to(per_feature, (owned, 128)).T[0:1, :] if owned == 128 else jnp.concatenate(
        [jnp.broadcast_to(per_feature, (owned, 128)).T[0:1, :], jnp.zeros((1, 128 - owned), f32)], axis=1
    )
    got_b[r] = msg_b[...]
    got_i[t] = msg_i[...]

    def tell_b(off):
        peer = lax.rem(r + off, R)
        return pltpu.make_async_remote_copy(
            msg_b, got_b.at[r], b_send.at[off], b_recv.at[r], device_id=(peer, t), device_id_type=MESH
        )

    def tell_i(off):
        peer = lax.rem(t + off, T)
        return pltpu.make_async_remote_copy(
            msg_i, got_i.at[t], i_send.at[off], i_recv.at[t], device_id=(r, peer), device_id_type=MESH
        )

    for off in range(1, R):
        tell_b(off).start()
    for off in range(1, T):
        tell_i(off).start()

    low = lane < 64
    for j in range(nbins // 2):
        base = 2 * j * width
        mid, end = pltpu.roll(at(2 * j + 1, 0), 64, 1), pltpu.roll(at(2 * j + 1, 1), 64, 1)
        child_ref[0, :, base : base + 128] = at(2 * j, 0)
        child_ref[0, :, base + 128 : base + 256] = jnp.where(low, at(2 * j, 1), mid)
        child_ref[0, :, base + 256 : base + 384] = jnp.where(low, mid, end)

    def drain(m, _):
        src = flip(m)
        direct(m, r).wait_send()

        @pl.when((m == 1) | (lax.rem(m, 2) == 0))
        def _():
            stats_out(m).wait_send()

        @pl.when(lax.rem(m, 2) == 0)
        def _():
            stats(src, flip(1), y_send).wait_send()

        relay(src, t, tx, x_send, x_recv).wait_send()
        relay(src, t, tp, p_send, p_recv).wait_send()
        relay(src, tx, tp, q_send, q_recv).wait_send()
        return 0

    lax.fori_loop(1, R, drain, 0)

    for off in range(1, T):
        src = lax.rem(t - off + T, T)
        pltpu.make_async_remote_copy(
            msg_i, got_i.at[src], i_send.at[off], i_recv.at[src], device_id=(r, src), device_id_type=MESH
        ).wait_recv()
    for off in range(1, R):
        src = lax.rem(r - off + R, R)
        pltpu.make_async_remote_copy(
            msg_b, got_b.at[src], b_send.at[off], b_recv.at[src], device_id=(src, t), device_id_type=MESH
        ).wait_recv()
    peak = got_b[0]
    for s in range(1, R):
        peak = jnp.maximum(peak, got_b[s])
    small_ref[:, 0:256] = peak
    tally = got_i[0]
    for s in range(1, T):
        tally = tally + got_i[s]
    small_ref[:, 256:384] = tally / (T * 2 * pairs)
    for off in range(1, T):
        tell_i(off).wait_send()
    for off in range(1, R):
        tell_b(off).wait_send()


def finish(owned, pairs, child_in, small_in, child_ref, best_ref, imp_ref, sem):
    out = pltpu.make_async_copy(child_in, child_ref, sem)
    out.start()
    width = 6 * pairs
    n_i = lax.broadcasted_iota(jnp.int32, (2 * pairs, width), 0)
    c_i = lax.broadcasted_iota(jnp.int32, (2 * pairs, width), 1)
    take = jnp.where(c_i == 3 * n_i, 1.0, 0.0)
    held = lax.rem(lax.broadcasted_iota(jnp.int32, (8, width), 1), 3) == 0
    peak = jnp.where(held, jnp.broadcast_to(small_in[:, 0:width], (8, width)), 0.0)
    best = lax.dot_general(peak, take, NT, precision=HIGH, preferred_element_type=jnp.float32)
    best_ref[...] = best[0:1, :]
    imp_ref[...] = small_in[:, 256 : 256 + owned]
    out.wait()


def fused(R, T, node_of_row, bag_weight, smaller_side, bins, target, parent_hist):
    nrows, feat = bins.shape
    pairs = smaller_side.shape[1]
    owned = feat // R
    quarter = nrows // T
    width = 6 * pairs
    f32, bf16 = jnp.float32, jnp.bfloat16
    vmem = pl.BlockSpec(memory_space=pltpu.VMEM)
    hbm = pl.BlockSpec(memory_space=pl.ANY)
    dma = pltpu.SemaphoreType.DMA
    child, small = pl.pallas_call(
        functools.partial(kernel, R, T, owned, BINS, pairs, nrows),
        out_shape=(pltpu.VMEM((1, owned, BINS * width), f32), pltpu.VMEM((1, 384), f32)),
        in_specs=[hbm, hbm, hbm, hbm, hbm, hbm],
        out_specs=(vmem, vmem),
        scratch_shapes=[
            pltpu.VMEM((1, nrows), jnp.int32),
            pltpu.VMEM((1, nrows), jnp.int32),
            pltpu.VMEM((1, nrows), f32),
            pltpu.VMEM((1, pairs), jnp.int32),
            pltpu.VMEM((quarter, feat), jnp.int32),
            pltpu.VMEM((nrows, 128), jnp.int32),
            pltpu.VMEM((T, 128, quarter), f32),
            pltpu.VMEM((R, owned, quarter), f32),
            pltpu.VMEM((R, T, owned, quarter), f32),
            pltpu.VMEM((R, 3 * nrows // 128, 128), f32),
            pltpu.VMEM((1, owned, BINS * 3 * pairs), f32),
            pltpu.VMEM((4, BINS // 4 * owned, 256), f32),
            pltpu.VMEM((256, quarter), bf16),
            pltpu.VMEM((width, quarter), bf16),
            pltpu.VMEM((width, quarter), bf16),
            pltpu.VMEM((1, 256), f32),
            pltpu.VMEM((R, 1, 256), f32),
            pltpu.VMEM((1, 128), f32),
            pltpu.VMEM((T, 1, 128), f32),
            dma((7,)), dma((R,)),
            dma((R,)), dma((R,)), dma((R,)), dma((R,)),
            dma((R,)), dma((R,)), dma((R,)), dma((R,)), dma((R,)), dma((R,)),
            dma((R,)), dma((R,)), dma((T,)), dma((T,)),
        ],
        compiler_params=pltpu.CompilerParams(collective_id=0, has_side_effects=True),
    )(*[pltpu.with_memory_space_constraint(x, pltpu.HBM) for x in (node_of_row, bag_weight, smaller_side, bins, target.reshape(1, nrows), parent_hist)])
    child, best, imp = pl.pallas_call(
        functools.partial(finish, owned, pairs),
        out_shape=(
            jax.ShapeDtypeStruct((1, owned, BINS * width), f32),
            jax.ShapeDtypeStruct((1, 2 * pairs), f32),
            jax.ShapeDtypeStruct((1, owned), f32),
        ),
        in_specs=[vmem, vmem],
        out_specs=(hbm, vmem, vmem),
        scratch_shapes=[dma],
        compiler_params=pltpu.CompilerParams(vmem_limit_bytes=8 << 20),
    )(pltpu.with_memory_space_constraint(child, pltpu.VMEM), pltpu.with_memory_space_constraint(small, pltpu.VMEM))
    return child, best, imp.reshape(owned)


def plain(node_of_row, bag_weight, smaller_side, bins, target, parent_hist):
    nrows = bins.shape[0]
    feat = bins.shape[1]
    pairs = smaller_side.shape[1]
    nbins = BINS
    nodes = node_of_row[0]
    flags = smaller_side[0]
    pair = nodes // 2
    side = nodes % 2
    pair_hot = pair[:, None] == jnp.arange(pairs, dtype=jnp.int32)[None, :]
    flag_row = jnp.sum(jnp.where(pair_hot, flags[None, :], 0), axis=1)
    keep = (side == flag_row).astype(jnp.float32)
    wk = bag_weight[0].astype(jnp.float32) * keep
    stats = jnp.stack([wk, wk * target, wk * target * target], axis=1).astype(jnp.bfloat16)
    spread = (pair_hot.astype(jnp.bfloat16)[:, :, None] * stats[:, None, :]).reshape(nrows, pairs * 3)
    levels = jnp.arange(nbins, dtype=jnp.int32)
    owned = feat // lax.axis_size("rows")
    width = math.gcd(lax.axis_size("rows") * owned, 32)

    def one_block(index):
        cols = lax.dynamic_slice_in_dim(bins, index * width, width, 1)
        onehot = (
            (cols[:, :, None] == levels[None, None, :]).astype(jnp.bfloat16).reshape(nrows, width * nbins)
        )
        part = jnp.einsum("rk,rm->km", onehot, spread, preferred_element_type=jnp.float32)
        return part.reshape(width, nbins * pairs * 3)

    blocks = lax.map(one_block, jnp.arange(lax.axis_size("rows") * owned // width, dtype=jnp.int32))
    small = lax.psum_scatter(
        blocks.reshape(lax.axis_size("rows") * owned, nbins * pairs * 3), "rows", scatter_dimension=0, tiled=True
    )
    small = small.reshape(owned, nbins, pairs, 3)
    parent = parent_hist[0].reshape(owned, nbins, pairs, 3)
    sibling = parent - small
    take = jnp.arange(2, dtype=jnp.int32)[None, :] == flags[:, None]
    children = jnp.where(take[None, None, :, :, None], small[:, :, :, None, :], sibling[:, :, :, None, :])
    children = children.reshape(owned, nbins, 2 * pairs, 3)
    ccum = jnp.cumsum(children[..., 0], axis=1)
    scum = jnp.cumsum(children[..., 1], axis=1)
    call = ccum[:, -1:, :]
    sall = scum[:, -1:, :]
    left_c = ccum[:, :-1, :]
    left_s = scum[:, :-1, :]
    gain = left_s * left_s / (jnp.maximum(left_c, 0.0) + 1.0)
    gain = gain + (sall - left_s) ** 2 / (jnp.maximum(call - left_c, 0.0) + 1.0)
    gain = gain - sall * sall / (jnp.maximum(call, 0.0) + 1.0)
    fgain = jnp.max(gain, axis=1)
    best = lax.pmax(jnp.max(fgain, axis=0), "rows")
    featsum = lax.psum(jnp.sum(fgain, axis=1), "trees")
    importance = featsum / (lax.axis_size("trees") * node_of_row.shape[0] * 2 * pairs)
    child_hist = children.reshape(owned, nbins * 2 * pairs * 3)
    return (child_hist[None], best[None], importance)


def solution(mesh):
    R, T = mesh.shape["rows"], mesh.shape["trees"]

    def shards(node_of_row, bag_weight, smaller_side, bins, target, parent_hist):
        nrows, feat = bins.shape
        pairs = smaller_side.shape[1]
        owned = feat // R
        fits = T == 4 and R % 2 == 0 and R & (R - 1) == 0 and node_of_row.shape[0] == 1
        fits = fits and R >= 4 and owned in (16, 32) and feat % 128 == 0 and nrows == T * 512
        fits = fits and pairs == 32 and R * nrows * owned * 4 <= 4 << 20
        body = functools.partial(fused, R, T) if fits else plain
        return body(node_of_row, bag_weight, smaller_side, bins, target, parent_hist)

    return jax.shard_map(
        shards,
        mesh=mesh,
        in_specs=(
            P("trees", "rows"),
            P("trees", "rows"),
            P("trees", None),
            P("rows", None),
            P("rows"),
            P("trees", "rows", None),
        ),
        out_specs=(P("trees", "rows", None), P("trees", None), P("rows")),
        check_vma=False,
    )
```
